32 devices in a mesh: gx: 4 (over x, core), gy: 8 (over z, y).
Axes of the slice: x: 2, y: 2, z: 4, core: 2. Of those that a mesh axis runs over, the one named last changes fastest.
Arguments:
- table: bfloat16 [32768, 512], P('gy'), may hold values from -40 to 40
- history: bfloat16 [2, 32, 1024, 512], P(None, 'gy', 'gx'), may hold values from -40 to 40
- lengths: int32 [8, 4], P('gy'), may hold values from 341 to 1024, as said below
- assignment: int32 [8, 4], P('gy'), may hold values from 0 to 3, each once within a row
- cand_owner: int32 [49152, 1], P(('gx', 'gy')), may hold values from 0 to 7; in each aligned block of 1536 rows (0 to 1535, 1536 to 3071, ...) at most 384 rows name the same one
- cand_row: int32 [49152], P(('gx', 'gy')), may hold values from 0 to 4095
- norm_gain: float32 [2, 512], replicated, may hold values from 0.1 to 1.9
- w_query: bfloat16 [2, 512, 1024], replicated, may hold values from -0.5 to 0.5
- w_key: bfloat16 [2, 512, 1024], replicated, may hold values from -1 to 1
- attn_gain: float32 [2, 512], replicated, may hold values from 0.1 to 1.9
- w_out: bfloat16 [2, 512, 512], replicated, may hold values from -0.25 to 0.25
Outputs:
- cand_out: bfloat16 [49152, 512], P(('gx', 'gy'))
The draws below stay inside these ranges and needn't reach their ends.
Inputs may be any that keep to these rules, and one draw needn't show every extreme that they name: `lengths`: some user has exactly 1024 live positions and some exactly 341. `assignment`: each row names each of its column's 4 users once. `cand_owner`: within the 1536 candidates of one device no table shard is named more than 384 times.
All inputs are finite; a program needn't handle non-finite values.
Results may differ from the reference program's by a relative error of at most 0.0075.
Values may be sent and summed in bfloat16 or wider, within the bound.
No kernel may reach another device: no remote copies, remote signals or barrier semaphores. Data moves between devices by JAX's collectives and lax.ppermute only.
A program may use at most 128 MiB of HBM per device.

```python
import math
import jax
import jax.numpy as jnp
import numpy as np
from jax import lax

D = 512
HEADS = 4
LAYERS = 2
LMAX = 1024
CAND = 1536
ROWS = 4096
CAP = 384
VOCAB = 32768
USERS = 32
TOTAL_CAND = 49152
N_GX = 4
N_GY = 8


def scaled_field(key, array_shape):
    key_rows, key_cols, key_base = jax.random.split(key, 3)
    row_shape = array_shape[:-1] + (1,)
    col_shape = (1,) * (len(array_shape) - 1) + (array_shape[-1],)
    row_scale = jnp.exp(jax.random.uniform(key_rows, row_shape, jnp.float32, math.log(0.3), math.log(3.0)))
    col_scale = jnp.exp(jax.random.uniform(key_cols, col_shape, jnp.float32, math.log(0.3), math.log(3.0)))
    base_draw = jax.random.normal(key_base, array_shape, jnp.float32)
    return jnp.clip(base_draw * row_scale * col_scale, -40.0, 40.0).astype(jnp.bfloat16)


def draw_table(key, part):
    return scaled_field(jax.random.fold_in(key, 11), (VOCAB, D))


def draw_history(key, part):
    return scaled_field(jax.random.fold_in(key, 12), (LAYERS, USERS, LMAX, D))


def draw_lengths(key, part):
    key_values, key_order = jax.random.split(jax.random.fold_in(key, 13))
    values_all = jax.random.randint(key_values, (USERS,), LMAX // 3, LMAX + 1, dtype=jnp.int32)
    user_order = jax.random.permutation(key_order, USERS)
    values_all = values_all.at[user_order[0]].set(LMAX).at[user_order[1]].set(LMAX // 3)
    return values_all.reshape(N_GY, N_GX).astype(jnp.int32)


def draw_w_key(key, part):
    key_base = jax.random.fold_in(key, 14)
    column_ids = jnp.arange(2 * D, dtype=jnp.int32)
    column_scale = jnp.where(column_ids < D, 0.5, 0.04).astype(jnp.float32) / math.sqrt(D)
    array_shape = (LAYERS, D, 2 * D)
    base_draw = jax.random.normal(key_base, array_shape, jnp.float32)
    return jnp.clip(base_draw * column_scale[None, None, :], -1.0, 1.0).astype(jnp.bfloat16)


def place_ends(array, own_key, smallest, largest):
    longest = array.shape.index(max(array.shape))
    spots = []
    for shift in (0, 1):
        where = [jax.random.randint(jax.random.fold_in(own_key, axis), (), 0, length) for axis, length in enumerate(array.shape)]
        where[longest] = (where[longest] + shift) % array.shape[longest]
        spots.append(tuple(where))
    return array.at[spots[0]].set(smallest).at[spots[1]].set(largest)


def rank_table(count, skew):
    loads = [(1 << 20) // math.isqrt(grade ** skew) + 1 for grade in range(1, count + 1)]
    deviation = 1 + sum(loads) // (1 << 30)
    return np.cumsum(np.array([max(1, weight // deviation) for weight in loads]))


def ranked_ids(key, shape, count, skew):
    table = rank_table(count, skew)
    ticket = jax.random.randint(jax.random.fold_in(key, 1), shape, 0, int(table[count - 1]))
    grade = jnp.searchsorted(jnp.asarray(table, jnp.int32), ticket, side="right")
    return jax.random.permutation(jax.random.fold_in(key, 2), count)[grade].astype(jnp.int32)


def shared_out(rng, own, number, rows, amount, top, most, skew):
    order = jax.random.permutation(rng, amount)
    crowded, common = load_shares(amount, rows * top, most, skew, True), load_shares(amount, rows * top, most, skew, False)
    places = jnp.arange(amount)

    def named(tallies, offset_by):
        used = int((tallies > 0).sum())
        fixed = max(1, used // 4)
        passed = fixed + (places - fixed + offset_by * (used - fixed)) % max(1, amount - fixed)
        return jnp.zeros((amount,), jnp.int32).at[order[jnp.where(places < fixed, places, passed)]].set(jnp.asarray(tallies, jnp.int32))

    tallies = jnp.where(number % 4 == 0, named(crowded, number // 4), named(common, number - number // 4 - 1))
    mixed = jax.random.permutation(jax.random.fold_in(own, 3), amount)
    source_of, taker = mixed[0:amount // 2 * 2:2], mixed[1:amount // 2 * 2:2]
    margin = jnp.minimum(tallies[source_of] - 1, most - tallies[taker]) // 2
    margin = jnp.where((source_of == order[0]) | (taker == order[0]) | (tallies[taker] == 0), 0, jnp.maximum(margin, 0))
    passed = jax.random.randint(jax.random.fold_in(own, 4), (amount // 2,), 0, 1 << 20) % (margin + 1)
    tallies = tallies.at[source_of].add(-passed).at[taker].add(passed)
    items = jnp.searchsorted(jnp.cumsum(tallies), jnp.arange(rows * top), side="right").astype(jnp.int32)
    grid = items.reshape(top, rows).T
    grid = grid[jax.random.permutation(jax.random.fold_in(own, 1), rows)]
    offset_by = jax.random.randint(jax.random.fold_in(own, 2), (rows, 1), 0, top)
    return jnp.take_along_axis(grid, (jnp.arange(top)[None, :] + offset_by) % top, axis=1)


def load_shares(amount, total, most, lean, full):
    loads = [(1 << 20) // math.isqrt(standing ** lean) + 1 for standing in range(1, amount + 1)]
    largest = most if full else min(most, max(-(-total // amount), total * loads[0] // sum(loads)))
    least = 1 if total - largest >= amount - 1 else 0
    counts, rest = [largest] + [least] * (amount - 1), total - largest - least * (amount - 1)
    while rest > 0:
        candidates = [i for i in range(1, amount) if counts[i] < largest] or [i for i in range(1, amount) if counts[i] < most]
        whole, left = sum([loads[i] for i in candidates]), rest
        for i in candidates:
            addition = min(most - counts[i], max(1, left * loads[i] // whole), rest)
            counts[i] = counts[i] + addition
            rest = rest - addition
    return np.array(counts)


def bell_draw(stream_key, extent, spread, bound, held_as=jnp.bfloat16):
    return jnp.clip(spread * jax.random.normal(stream_key, extent, jnp.float32), -bound, bound).astype(held_as)


def setup_inputs(seed: int = 0) -> dict:
    keys = jax.random.split(jax.random.key(seed), 12)
    table = draw_table(jax.random.fold_in(keys[11], 71), 0)
    history = draw_history(jax.random.fold_in(keys[11], 71), 0)
    lengths = draw_lengths(jax.random.fold_in(keys[11], 71), 0)
    assignment = jax.vmap(lambda own: jax.random.permutation(own, N_GX))(jax.random.split(keys[3], N_GY)).reshape((N_GY, N_GX)).astype(jnp.int32)
    cand_owner_keys = jax.random.split(jax.random.fold_in(keys[4], 1), TOTAL_CAND // CAND)
    cand_owner_turns = jax.random.permutation(jax.random.fold_in(keys[4], 3), TOTAL_CAND // CAND)
    cand_owner = jax.vmap(lambda own, number: shared_out(jax.random.fold_in(keys[4], 2), own, number, CAND, N_GY, 1, CAP, 2))(cand_owner_keys, cand_owner_turns).reshape((TOTAL_CAND, 1))
    cand_row = place_ends(ranked_ids(keys[5], (TOTAL_CAND,), ROWS, 2), jax.random.fold_in(keys[5], 3), 0, ROWS - 1).astype(jnp.int32)
    norm_gain = jnp.clip(1.0 + 0.18 * jax.random.normal(keys[6], (LAYERS, D), jnp.float32), 0.1, 1.9)
    w_query = bell_draw(keys[7], (LAYERS, D, 2 * D), (D // 4) ** -0.5, 0.5)
    w_key = draw_w_key(jax.random.fold_in(keys[11], 71), 0)
    attn_gain = jnp.clip(1.0 + 0.18 * jax.random.normal(keys[9], (LAYERS, D), jnp.float32), 0.1, 1.9)
    w_out = bell_draw(keys[10], (LAYERS, D, D), D ** -0.5, 0.25)
    return {"table": table, "history": history, "lengths": lengths, "assignment": assignment, "cand_owner": cand_owner, "cand_row": cand_row, "norm_gain": norm_gain, "w_query": w_query, "w_key": w_key, "attn_gain": attn_gain, "w_out": w_out}


epsilon = 1e-06

def rms_scale(vector, gain_row):
    return vector * lax.rsqrt(lax.optimization_barrier(jnp.mean(vector * vector, axis=-1, keepdims=True)) + epsilon) * gain_row

def attend(query_part, key_rows, value_rows, live_mask):
    head_size = D // HEADS
    count_rows = query_part.shape[0]
    queries = query_part.astype(jnp.float32).reshape(count_rows, HEADS, head_size)
    keyed = key_rows.astype(jnp.float32).reshape(LMAX, HEADS, head_size)
    valued = value_rows.astype(jnp.float32).reshape(LMAX, HEADS, head_size)
    scores = jnp.einsum('chd,lhd->hcl', queries, keyed) * head_size ** (-0.5)
    weights = jnp.where(live_mask[None, None, :], jax.nn.silu(scores), 0.0).astype(jnp.bfloat16)
    attended = jnp.einsum('hcl,lhd->chd', weights.astype(jnp.float32), valued)
    return attended.reshape(count_rows, D)

def score_request(embedded_rows, user_history, length, norm_gain, w_query, w_key, attn_gain, w_out):
    stream = embedded_rows.astype(jnp.float32)
    live_mask = jnp.arange(LMAX, dtype=jnp.int32) < length
    for layer_index in range(LAYERS):
        normed = rms_scale(stream, norm_gain[layer_index]).astype(jnp.bfloat16)
        gate_query = jax.nn.silu(jnp.dot(normed, w_query[layer_index], preferred_element_type=jnp.float32)).astype(jnp.bfloat16)
        history_normed = rms_scale(user_history[layer_index].astype(jnp.float32), norm_gain[layer_index]).astype(jnp.bfloat16)
        key_value = jax.nn.silu(jnp.dot(history_normed, w_key[layer_index], preferred_element_type=jnp.float32)).astype(jnp.bfloat16)
        attended = attend(gate_query[:, D:], key_value[:, :D], key_value[:, D:], live_mask)
        gated_out = (rms_scale(attended, attn_gain[layer_index]) * gate_query[:, :D].astype(jnp.float32)).astype(jnp.bfloat16)
        stream = stream + jnp.dot(gated_out, w_out[layer_index], preferred_element_type=jnp.float32)
    return stream.astype(jnp.bfloat16)

def reference(table, history, lengths, assignment, cand_owner, cand_row, norm_gain, w_query, w_key, attn_gain, w_out):
    global_rows = (cand_owner[:, 0] * ROWS + cand_row).astype(jnp.int32)
    embedded = jnp.take(table, global_rows, axis=0).reshape(N_GX * N_GY, CAND, D)
    device_ids = jnp.arange(N_GX * N_GY, dtype=jnp.int32)
    across = device_ids // N_GY
    column = device_ids % N_GY
    slot_index = assignment[column, across].astype(jnp.int32)
    user_index = (column * N_GX + slot_index).astype(jnp.int32)
    live_length = lengths[column, slot_index].astype(jnp.int32)

    def one_device(packed):
        embedded_rows, who, length = packed
        user_history = lax.dynamic_index_in_dim(history, who, axis=1, keepdims=False)
        return score_request(embedded_rows, user_history, length, norm_gain, w_query, w_key, attn_gain, w_out)
    scored = lax.map(one_device, (embedded, user_index, live_length))
    return scored.reshape(N_GX * N_GY * CAND, D)
```

```python
import functools

import jax
import jax.numpy as jnp
from jax import lax
from jax.experimental import pallas as pl
from jax.experimental.pallas import tpu as pltpu
from jax.sharding import PartitionSpec as P

HEADS = 4
EPSILON = 1e-06
NT = (((1,), (1,)), ((), ()))
KEY_TILE = 256
VMEM_LIMIT = 60 * 2**20
F32, BF16 = jnp.float32, jnp.bfloat16


def half_silu(half):
    return half + half * jnp.tanh(half)


def rms_scale(vector, gain_row):
    scale = lax.rsqrt(jnp.mean(vector * vector, axis=-1, keepdims=True) + EPSILON)
    return vector * scale * gain_row


def params(*semantics):
    return pltpu.CompilerParams(
        dimension_semantics=semantics or None, vmem_limit_bytes=VMEM_LIMIT
    )


def cost(flops, moved):
    return pl.CostEstimate(flops=int(flops), bytes_accessed=int(moved), transcendentals=0)


def iota(shape, axis):
    return lax.broadcasted_iota(jnp.int32, shape, axis).astype(F32)


def column(row):
    return jnp.broadcast_to(row, (8, row.shape[1])).T[:, 0:1]


def requests_kernel(rows, fast_cap, first_cap, first_count, owner_ref, row_ref, req_ref, rank_ref):
    groups, capacity = req_ref.shape
    count = owner_ref.shape[1]
    owner = owner_ref[...].astype(F32)
    row = row_ref[...].astype(F32)
    key = owner * rows + row
    keys = column(key)
    place = iota((1, count), 1)
    step = 128
    first = jnp.full((8, count), float(count), F32)
    for base in range(0, count, step):
        same = keys[base : base + step] == key
        at = jnp.where(same, iota((step, 1), 0) + base, float(count))
        first = jnp.minimum(first, jnp.min(at.reshape(step // 8, 8, count), axis=0))
    first = jnp.min(first, axis=0, keepdims=True)
    owned = iota((groups, 1), 0) == owner
    leads = jnp.where(owned & (first == place), 1.0, 0.0)
    prior = jnp.zeros((groups, count), F32)
    step = 256
    for base in range(0, count, step):
        before = jnp.where(iota((step, 1), 0) + base < first, 1.0, 0.0).astype(BF16)
        prior += jnp.dot(
            leads[:, base : base + step].astype(BF16), before, preferred_element_type=F32
        )
    rank = jnp.sum(jnp.where(owned, prior, 0.0), axis=0, keepdims=True)
    high = jnp.floor(row * (1.0 / 256))
    low = row - high * 256
    parts = jnp.concatenate([leads * high, leads * low], axis=0).astype(BF16)
    at_slot = jnp.where(iota((capacity, 1), 0) == rank, 1.0, 0.0).astype(BF16)
    listed = lax.dot_general(parts, at_slot, NT, preferred_element_type=F32)
    asked = listed[:groups] * 256 + listed[groups:]
    most = jnp.max(jnp.sum(leads, axis=1, keepdims=True), axis=0, keepdims=True)
    ready = jnp.sum(jnp.where(rank < first_cap, 1.0, 0.0), axis=1, keepdims=True)
    slow = (most > fast_cap) | (ready < first_count)
    req_ref[...] = (asked + jnp.where(slow, float(rows), 0.0)).astype(jnp.int32)
    rank_ref[...] = rank.astype(jnp.int32)


def order_kernel(groups, fast_cap, first_cap, owner_ref, rank_ref, pos_ref, slot_ref):
    count = owner_ref.shape[1]
    owner = owner_ref[...].astype(F32)
    rank = rank_ref[...].astype(F32)
    key = rank * count + iota((1, count), 1)
    keys = column(key)
    step = 128
    smaller = jnp.zeros((8, count), F32)
    for base in range(0, count, step):
        less = jnp.where(keys[base : base + step] < key, 1.0, 0.0)
        smaller += jnp.sum(less.reshape(step // 8, 8, count), axis=0)
    pos = jnp.sum(smaller, axis=0, keepdims=True)
    pos_ref[...] = column(pos)
    rest = fast_cap - first_cap
    slot = jnp.where(
        rank < first_cap,
        owner * first_cap + rank,
        groups * first_cap + owner * rest + (rank - first_cap),
    )
    for base in range(0, count, step):
        here = jnp.where(iota((step, 1), 0) + base == pos, slot, 0.0)
        slot_ref[base : base + step, :] = jnp.sum(here, axis=1, keepdims=True)


def lookup_kernel(offset, ids_ref, table_ref, out_ref, select):
    groups, length, _ = out_ref.shape
    rows = table_ref.shape[0]
    ids = ids_ref[...].astype(F32)
    ids = jnp.where(ids >= rows, ids - rows, ids)
    columns = ids.T[offset : offset + length]
    lanes = iota((1, rows), 1)
    part = groups // 2
    for base in range(0, groups, part):
        for g in range(part):
            hit = columns[:, base + g : base + g + 1] == lanes
            select[g * length : (g + 1) * length, :] = jnp.where(hit, 1.0, 0.0).astype(BF16)
        found = jnp.dot(select[...], table_ref[...], preferred_element_type=F32)
        out_ref[base : base + part] = found.astype(BF16).reshape(part, length, -1)


def lookup(ids, table, offset, length):
    groups = ids.shape[0]
    rows, features = table.shape
    return pl.pallas_call(
        functools.partial(lookup_kernel, offset),
        out_shape=jax.ShapeDtypeStruct((groups, length, features), BF16),
        scratch_shapes=[pltpu.VMEM((groups // 2 * length, rows), BF16)],
        compiler_params=params(),
        cost_estimate=cost(2 * groups * length * rows * features, table.size * 2),
        name="lookup",
    )(ids, table)


def pick_kernel(count, slot_ref, *refs):
    out_ref = refs[count]
    slot = slot_ref[...]
    total = None
    base = 0
    for ref in refs[:count]:
        size = ref.shape[0]
        hit = jnp.where(slot == iota((1, size), 1) + base, 1.0, 0.0).astype(BF16)
        found = jnp.dot(hit, ref[...], preferred_element_type=F32)
        total = found if total is None else total + found
        base += size
    out_ref[...] = total.astype(out_ref.dtype)


def pick(slots, sources, first, amount, tile):
    features = sources[0].shape[1]
    lead = first // tile
    size = sum(source.shape[0] for source in sources)
    return pl.pallas_call(
        functools.partial(pick_kernel, len(sources)),
        grid=(amount // tile,),
        in_specs=[pl.BlockSpec((tile, 1), lambda i: (i + lead, 0))]
        + [pl.BlockSpec(source.shape, lambda i: (0, 0)) for source in sources],
        out_specs=pl.BlockSpec((tile, features), lambda i: (i, 0)),
        out_shape=jax.ShapeDtypeStruct((amount, features), BF16),
        compiler_params=params("arbitrary"),
        cost_estimate=cost(2 * amount * size * features, size * features * 2),
        name="pick",
    )(slots, *sources)


def history_kernel(members, assignment_ref, history_ref, *refs):
    outs, sems = refs[:-1], refs[-1]
    own = lax.axis_index("gx")
    copies = []
    for shift, out in enumerate(outs, 1):
        user = assignment_ref[0, lax.rem(own + shift, members)]
        copies.append(pltpu.make_async_copy(history_ref.at[:, user], out, sems.at[shift - 1]))
    for copy in copies:
        copy.start()
    for copy in copies:
        copy.wait()


def history_blocks(assignment, history, members):
    layers, _, span, features = history.shape
    block = jax.ShapeDtypeStruct((layers, span, features), BF16)
    return pl.pallas_call(
        functools.partial(history_kernel, members),
        in_specs=[
            pl.BlockSpec(memory_space=pltpu.SMEM),
            pl.BlockSpec(memory_space=pl.ANY),
        ],
        out_specs=[pl.BlockSpec(memory_space=pltpu.VMEM)] * (members - 1),
        out_shape=[block] * (members - 1),
        scratch_shapes=[pltpu.SemaphoreType.DMA((members - 1,))],
        compiler_params=params(),
        cost_estimate=cost(1, history.size * 4),
        name="history_blocks",
    )(assignment, history)


def project_kernel(members, assignment_ref, lengths_ref, history_ref, *refs):
    blocks = refs[: members - 1]
    gain_ref, weight_ref, key_ref, value_ref, own_block, sem = refs[members - 1 :]
    span, features = own_block.shape
    layer = pl.program_id(0)
    own = lax.axis_index("gx")
    user = assignment_ref[0, own]
    length = lengths_ref[0, user]
    copy = pltpu.make_async_copy(history_ref.at[layer, user], own_block, sem)
    copy.start()
    copy.wait()
    for shift in range(members):
        states = own_block[...] if shift == 0 else blocks[shift - 1][0]
        normed = rms_scale(states.astype(F32), gain_ref[0]).astype(BF16)
        half = 0.5 * jnp.dot(normed, weight_ref[0], preferred_element_type=F32)
        key_value = half_silu(half)
        start = pl.multiple_of(lax.rem(own - shift + members, members) * span, span)
        live = lax.broadcasted_iota(jnp.int32, (span, 1), 0) + start < length
        key_ref[0, pl.ds(start, span), :] = key_value[:, :features].astype(BF16)
        value = jnp.where(live, key_value[:, features:], 0.0)
        value_ref[0, pl.ds(start, span), :] = value.astype(BF16)


def project(assignment, lengths, history, blocks, gain, weight):
    layers, _, span, features = history.shape
    members = len(blocks) + 1
    per_layer = lambda *shape: pl.BlockSpec((1,) + shape, lambda i: (i, 0, 0))
    whole = jax.ShapeDtypeStruct((layers, span * members, features), BF16)
    return pl.pallas_call(
        functools.partial(project_kernel, members),
        grid=(layers,),
        in_specs=[
            pl.BlockSpec(memory_space=pltpu.SMEM),
            pl.BlockSpec(memory_space=pltpu.SMEM),
            pl.BlockSpec(memory_space=pl.ANY),
        ]
        + [per_layer(span, features)] * (members - 1)
        + [per_layer(1, features), per_layer(features, 2 * features)],
        out_specs=[per_layer(span * members, features)] * 2,
        out_shape=[whole] * 2,
        scratch_shapes=[pltpu.VMEM((span, features), BF16), pltpu.SemaphoreType.DMA],
        compiler_params=params("arbitrary"),
        cost_estimate=cost(4 * layers * span * members * features**2, history.size * 4),
        name="project",
    )(assignment, lengths, history, *blocks, gain.reshape(layers, 1, features), weight)


def layers_kernel(x_ref, key_ref, value_ref, ng_ref, wq_ref, ag_ref, wo_ref, out_ref):
    layers, total, features = key_ref.shape
    size = features // HEADS
    scale = 0.5 * size**-0.5
    x = x_ref[...].astype(F32)
    for layer in range(layers):
        normed = rms_scale(x, ng_ref[layer : layer + 1, :]).astype(BF16)
        weight = wq_ref[layer]
        gate = jnp.dot(normed, weight[:, :features], preferred_element_type=F32)
        gate = half_silu(0.5 * gate).astype(BF16)
        query = jnp.dot(normed, weight[:, features:], preferred_element_type=F32)
        query = (half_silu(0.5 * query) * scale).astype(BF16)
        heads = []
        for head in range(HEADS):
            columns = slice(head * size, (head + 1) * size)
            attended = None
            for base in range(0, total, KEY_TILE):
                rows = slice(base, base + KEY_TILE)
                half = lax.dot_general(
                    query[:, columns],
                    key_ref[layer, rows, columns],
                    NT,
                    preferred_element_type=F32,
                )
                part = jnp.dot(
                    half_silu(half).astype(BF16),
                    value_ref[layer, rows, columns],
                    preferred_element_type=F32,
                )
                attended = part if attended is None else attended + part
            heads.append(attended)
        attended = rms_scale(jnp.concatenate(heads, axis=1), ag_ref[layer : layer + 1, :])
        gated = (attended * gate.astype(F32)).astype(BF16)
        x = x + jnp.dot(gated, wo_ref[layer], preferred_element_type=F32)
    out_ref[...] = x.astype(BF16)


def run_layers(x, tile, keys, values, norm_gain, w_query, attn_gain, w_out):
    amount, features = x.shape
    layers, total, _ = keys.shape
    full = lambda a: pl.BlockSpec(a.shape, lambda i: (0,) * a.ndim)
    shared = (keys, values, norm_gain, w_query, attn_gain, w_out)
    flops = layers * amount * features * (6 * features + 8 * total)
    return pl.pallas_call(
        layers_kernel,
        grid=(amount // tile,),
        in_specs=[pl.BlockSpec((tile, features), lambda i: (i, 0))] + [full(a) for a in shared],
        out_specs=pl.BlockSpec((tile, features), lambda i: (i, 0)),
        out_shape=jax.ShapeDtypeStruct((amount, features), BF16),
        compiler_params=params("arbitrary"),
        cost_estimate=cost(flops, keys.size * 8),
        name="run_layers",
    )(x, *shared)


def local(
    table,
    history,
    lengths,
    assignment,
    cand_owner,
    cand_row,
    norm_gain,
    w_query,
    w_key,
    attn_gain,
    w_out,
):
    groups = lax.axis_size("gy")
    members = lax.axis_size("gx")
    count = cand_row.shape[0]
    rows, features = table.shape
    capacity = 2 * count // groups
    fast_cap = 2 * capacity // 3
    first_cap = capacity // 3
    tile = count // 4
    first_count = 3 * tile

    owner = cand_owner.reshape(1, count)
    row = cand_row.reshape(1, count)
    requests, rank = pl.pallas_call(
        functools.partial(requests_kernel, rows, fast_cap, first_cap, first_count),
        out_shape=[
            jax.ShapeDtypeStruct((groups, capacity), jnp.int32),
            jax.ShapeDtypeStruct((1, count), jnp.int32),
        ],
        compiler_params=params(),
        cost_estimate=cost(8 * count * count, 1),
        name="requests",
    )(owner, row)

    def exchange(block):
        return lax.all_to_all(block, "gy", split_axis=0, concat_axis=0, tiled=True)

    ids = exchange(requests)
    slow = jnp.any(ids >= rows)

    sent = history_blocks(assignment, history, members)
    blocks = [
        lax.ppermute(block, "gx", [(j, (j + shift) % members) for j in range(members)])
        for shift, block in enumerate(sent, 1)
    ]
    pos, slots = pl.pallas_call(
        functools.partial(order_kernel, groups, fast_cap, first_cap),
        out_shape=[jax.ShapeDtypeStruct((count, 1), F32)] * 2,
        compiler_params=params(),
        cost_estimate=cost(8 * count * count, 1),
        name="order",
    )(owner, rank)

    arrived_1 = exchange(lookup(ids, table, 0, first_cap)).reshape(groups * first_cap, features)
    arrived_2 = exchange(lookup(ids, table, first_cap, fast_cap - first_cap))
    arrived_2 = arrived_2.reshape(groups * (fast_cap - first_cap), features)
    keys, values = project(assignment, lengths, history, blocks, norm_gain, w_key)
    shared = (keys, values, norm_gain, w_query, attn_gain, w_out)
    early = run_layers(pick(slots, (arrived_1,), 0, first_count, tile), tile, *shared)
    late = pick(slots, (arrived_1, arrived_2), first_count, count - first_count, tile)
    late = run_layers(late, tile, *shared)

    def in_order(operands):
        return pick(operands[0], (operands[1], operands[2]), 0, count, tile)

    def in_full(operands):
        asked = jnp.where(ids >= rows, ids - rows, ids)
        arrived = exchange(jnp.take(table, asked, axis=0, mode="clip"))
        place = (owner * capacity + rank).reshape(count)
        embedded = jnp.take(arrived.reshape(groups * capacity, features), place, axis=0, mode="clip")
        return run_layers(embedded, tile, *shared)

    return lax.cond(slow, in_full, in_order, (pos, early, late))


def solution(mesh):
    return jax.shard_map(
        local,
        mesh=mesh,
        in_specs=(
            P("gy", None),
            P(None, "gy", "gx", None),
            P("gy", None),
            P("gy", None),
            P(("gx", "gy"), None),
            P(("gx", "gy")),
            P(),
            P(),
            P(),
            P(),
            P(),
        ),
        out_specs=P(("gx", "gy"), None),
        check_vma=False,
    )
```

```python
import functools

import jax
import jax.numpy as jnp
from jax import lax
from jax.experimental import pallas as pl
from jax.experimental.pallas import tpu as pltpu
from jax.sharding import PartitionSpec as P


HEADS = 4
EPSILON = 1e-06
NT = (((1,), (1,)), ((), ()))
KEY_TILE = 256
LANES = 128
F32, BF16 = jnp.float32, jnp.bfloat16


def half_silu(half):
    return half + half * jnp.tanh(half)


def rms_scale(vector, gain_row):
    scale = lax.rsqrt(jnp.mean(vector * vector, axis=-1, keepdims=True) + EPSILON)
    return vector * scale * gain_row


def params(mib, *semantics):
    return pltpu.CompilerParams(
        dimension_semantics=semantics or None, vmem_limit_bytes=mib * 2**20
    )


def cost(flops, moved):
    return pl.CostEstimate(flops=int(flops), bytes_accessed=int(moved), transcendentals=0)


def iota(shape, axis):
    return lax.broadcasted_iota(jnp.int32, shape, axis).astype(F32)


def column(row):
    return jnp.broadcast_to(row, (8, row.shape[1])).T[:, 0:1]


def requests_kernel(
    rows,
    members,
    fast_cap,
    first_cap,
    first_count,
    owner_ref,
    row_ref,
    assignment_ref,
    history_ref,
    req_ref,
    rank_ref,
    *refs,
):
    sent, (held, read_sems, write_sems) = refs[: members - 1], refs[members - 1 :]
    own = lax.axis_index("gx")
    reads, writes = [], []
    for shift, out in enumerate(sent, 1):
        user = assignment_ref[0, lax.rem(own + shift, members)]
        block = held.at[shift - 1]
        reads.append(
            pltpu.make_async_copy(history_ref.at[:, user], block, read_sems.at[shift - 1])
        )
        writes.append(pltpu.make_async_copy(block, out, write_sems.at[shift - 1]))
    for copy in reads:
        copy.start()
    groups = req_ref.shape[0]
    capacity = req_ref.shape[2] - LANES
    count = owner_ref.shape[1]
    owner = owner_ref[...].astype(F32)
    row = row_ref[...].astype(F32)
    key = owner * rows + row
    keys = column(key)
    place = iota((1, count), 1)
    step = 128
    first = jnp.full((8, count), float(count), F32)
    for base in range(0, count, step):
        same = keys[base : base + step] == key
        at = jnp.where(same, iota((step, 1), 0) + base, float(count))
        first = jnp.minimum(first, jnp.min(at.reshape(step // 8, 8, count), axis=0))
    first = jnp.min(first, axis=0, keepdims=True)
    for read, write in zip(reads, writes):
        read.wait()
        write.start()
    owned = iota((groups, 1), 0) == owner
    leads = jnp.where(owned & (first == place), 1.0, 0.0)
    prior = jnp.zeros((groups, count), F32)
    step = 256
    for base in range(0, count, step):
        before = jnp.where(iota((step, 1), 0) + base < first, 1.0, 0.0).astype(BF16)
        prior += jnp.dot(
            leads[:, base : base + step].astype(BF16), before, preferred_element_type=F32
        )
    rank = jnp.sum(jnp.where(owned, prior, 0.0), axis=0, keepdims=True)
    high = jnp.floor(row * (1.0 / 256))
    low = row - high * 256
    parts = jnp.concatenate([leads * high, leads * low], axis=0).astype(BF16)
    at_slot = jnp.where(iota((capacity, 1), 0) == rank, 1.0, 0.0).astype(BF16)
    listed = lax.dot_general(parts, at_slot, NT, preferred_element_type=F32)
    asked = listed[:groups] * 256 + listed[groups:]
    most = jnp.max(jnp.sum(leads, axis=1, keepdims=True), axis=0, keepdims=True)
    ready = jnp.sum(jnp.where(rank < first_cap, 1.0, 0.0), axis=1, keepdims=True)
    slow = (most > fast_cap) | (ready < first_count)
    flag = jnp.broadcast_to(jnp.where(slow, 1, 0).astype(jnp.int32), (1, LANES))
    asked = asked.astype(jnp.int32)
    for g in range(groups):
        req_ref[g, :, :capacity] = asked[g : g + 1]
        req_ref[g, :, capacity:] = flag
    rank_ref[...] = rank.astype(jnp.int32)
    for write in writes:
        write.wait()


def order_kernel(groups, fast_cap, first_cap, owner_ref, rank_ref, pos_ref, slot_ref):
    count = owner_ref.shape[1]
    owner = owner_ref[...].astype(F32)
    rank = rank_ref[...].astype(F32)
    key = rank * count + iota((1, count), 1)
    keys = column(key)
    step = 128
    smaller = jnp.zeros((8, count), F32)
    for base in range(0, count, step):
        less = jnp.where(keys[base : base + step] < key, 1.0, 0.0)
        smaller += jnp.sum(less.reshape(step // 8, 8, count), axis=0)
    pos = jnp.sum(smaller, axis=0, keepdims=True)
    pos_ref[...] = column(pos)
    rest = fast_cap - first_cap
    slot = jnp.where(
        rank < first_cap,
        owner * first_cap + rank,
        groups * first_cap + owner * rest + (rank - first_cap),
    )
    for base in range(0, count, step):
        here = jnp.where(iota((step, 1), 0) + base == pos, slot, 0.0)
        slot_ref[base : base + step, :] = jnp.sum(here, axis=1, keepdims=True)


def lookup_kernel(offset, ids_ref, table_ref, _, out_ref, select):
    groups, length, features = out_ref.shape
    lanes = iota((1, table_ref.shape[0]), 1)
    for g in range(groups):
        ids = column(ids_ref[g].astype(F32))[offset : offset + length]
        hit = jnp.where(ids == lanes, 1.0, 0.0)
        select[g * length : (g + 1) * length, :] = hit.astype(BF16)
    found = jnp.dot(select[...], table_ref[...], preferred_element_type=F32)
    out_ref[...] = found.astype(BF16).reshape(groups, length, features)


def lookup(ids, table, after, offset, length):
    groups = ids.shape[0]
    rows, features = table.shape
    whole = lambda a: pl.BlockSpec(a.shape, lambda i: (0,) * a.ndim)
    return pl.pallas_call(
        functools.partial(lookup_kernel, offset),
        grid=(1,),
        in_specs=[whole(ids), whole(table), pl.BlockSpec(after.shape if after.shape[0] < 8 else (8, after.shape[1]), lambda i: (0, 0))],
        out_specs=pl.BlockSpec((groups, length, features), lambda i: (0, 0, 0)),
        out_shape=jax.ShapeDtypeStruct((groups, length, features), BF16),
        scratch_shapes=[pltpu.VMEM((groups * length, rows), BF16)],
        compiler_params=params(30, "arbitrary"),
        cost_estimate=cost(2 * groups * length * rows * features, table.size * 2),
        name="lookup",
    )(ids, table, after)


def pick_kernel(base, count, added, slot_ref, *refs):
    out_ref = refs[-1]
    slot = slot_ref[...]
    total = None
    for ref in refs[:count]:
        size = ref.shape[0]
        hit = jnp.where(slot == iota((1, size), 1) + base, 1.0, 0.0).astype(BF16)
        found = jnp.dot(hit, ref[...], preferred_element_type=F32)
        total = found if total is None else total + found
        base += size
    if added:
        total = total + refs[count][...].astype(F32)
    out_ref[...] = total.astype(out_ref.dtype)


def pick(slots, sources, base, first, amount, tile, addend=None, after=None):
    features = sources[0].shape[1]
    lead = first // tile
    size = sum(source.shape[0] for source in sources)
    row_block = pl.BlockSpec((tile, features), lambda i: (i, 0))
    return pl.pallas_call(
        functools.partial(pick_kernel, base, len(sources), addend is not None),
        grid=(amount // tile,),
        in_specs=[pl.BlockSpec((tile, 1), lambda i: (i + lead, 0))]
        + [pl.BlockSpec(source.shape, lambda i: (0, 0)) for source in sources]
        + ([] if addend is None else [row_block])
        + ([] if after is None else [pl.BlockSpec((16, features), lambda i: (0, 0))]),
        out_specs=row_block,
        out_shape=jax.ShapeDtypeStruct((amount, features), BF16),
        compiler_params=params(16, "arbitrary"),
        cost_estimate=cost(2 * amount * size * features, size * features * 2),
        name="pick",
    )(slots, *sources, *[x for x in (addend, after) if x is not None])


def project_kernel(members, assignment_ref, lengths_ref, history_ref, *refs):
    blocks = refs[: members - 1]
    gain_ref, weight_ref, key_ref, value_ref, own_block, sem = refs[members - 1 :]
    span, features = own_block.shape
    layer = pl.program_id(0)
    own = lax.axis_index("gx")
    user = assignment_ref[0, own]
    length = lengths_ref[0, user]
    copy = pltpu.make_async_copy(history_ref.at[layer, user], own_block, sem)
    copy.start()
    copy.wait()
    for shift in range(members):
        states = own_block[...] if shift == 0 else blocks[shift - 1][0]
        normed = rms_scale(states.astype(F32), gain_ref[0]).astype(BF16)
        half = 0.5 * jnp.dot(normed, weight_ref[0], preferred_element_type=F32)
        key_value = half_silu(half)
        start = pl.multiple_of(lax.rem(own - shift + members, members) * span, span)
        live = lax.broadcasted_iota(jnp.int32, (span, 1), 0) + start < length
        key_ref[0, pl.ds(start, span), :] = key_value[:, :features].astype(BF16)
        value = jnp.where(live, key_value[:, features:], 0.0)
        value_ref[0, pl.ds(start, span), :] = value.astype(BF16)


def project(assignment, lengths, history, blocks, gain, weight):
    layers, _, span, features = history.shape
    members = len(blocks) + 1
    per_layer = lambda *shape: pl.BlockSpec((1,) + shape, lambda i: (i, 0, 0))
    whole = jax.ShapeDtypeStruct((layers, span * members, features), BF16)
    return pl.pallas_call(
        functools.partial(project_kernel, members),
        grid=(layers,),
        in_specs=[
            pl.BlockSpec(memory_space=pltpu.SMEM),
            pl.BlockSpec(memory_space=pltpu.SMEM),
            pl.BlockSpec(memory_space=pltpu.HBM),
        ]
        + [per_layer(span, features)] * (members - 1)
        + [per_layer(1, features), per_layer(features, 2 * features)],
        out_specs=[per_layer(span * members, features)] * 2,
        out_shape=[whole] * 2,
        scratch_shapes=[pltpu.VMEM((span, features), BF16), pltpu.SemaphoreType.DMA],
        compiler_params=params(20, "arbitrary"),
        cost_estimate=cost(4 * layers * span * members * features**2, history.size * 4),
        name="project",
    )(assignment, lengths, history, *blocks, gain.reshape(layers, 1, features), weight)


def layers_kernel(x_ref, key_ref, value_ref, ng_ref, wq_ref, ag_ref, wo_ref, out_ref):
    layers, total, features = key_ref.shape
    size = features // HEADS
    scale = 0.5 * size**-0.5
    x = x_ref[...].astype(F32)
    for layer in range(layers):
        normed = rms_scale(x, ng_ref[layer : layer + 1, :]).astype(BF16)
        weight = wq_ref[layer]
        gate = jnp.dot(normed, weight[:, :features], preferred_element_type=F32)
        gate = half_silu(0.5 * gate).astype(BF16)
        query = jnp.dot(normed, weight[:, features:], preferred_element_type=F32)
        query = (half_silu(0.5 * query) * scale).astype(BF16)
        heads = []
        for head in range(HEADS):
            columns = slice(head * size, (head + 1) * size)
            attended = None
            for base in range(0, total, KEY_TILE):
                rows = slice(base, base + KEY_TILE)
                half = lax.dot_general(
                    query[:, columns],
                    key_ref[layer, rows, columns],
                    NT,
                    preferred_element_type=F32,
                )
                part = jnp.dot(
                    half_silu(half).astype(BF16),
                    value_ref[layer, rows, columns],
                    preferred_element_type=F32,
                )
                attended = part if attended is None else attended + part
            heads.append(attended)
        attended = rms_scale(jnp.concatenate(heads, axis=1), ag_ref[layer : layer + 1, :])
        gated = (attended * gate.astype(F32)).astype(BF16)
        x = x + jnp.dot(gated, wo_ref[layer], preferred_element_type=F32)
    out_ref[...] = x.astype(BF16)


def run_layers(x, tile, keys, values, norm_gain, w_query, attn_gain, w_out):
    amount, features = x.shape
    layers, total, _ = keys.shape
    full = lambda a: pl.BlockSpec(a.shape, lambda i: (0,) * a.ndim)
    shared = (keys, values, norm_gain, w_query, attn_gain, w_out)
    flops = layers * amount * features * (6 * features + 8 * total)
    return pl.pallas_call(
        layers_kernel,
        grid=(amount // tile,),
        in_specs=[pl.BlockSpec((tile, features), lambda i: (i, 0))] + [full(a) for a in shared],
        out_specs=pl.BlockSpec((tile, features), lambda i: (i, 0)),
        out_shape=jax.ShapeDtypeStruct((amount, features), BF16),
        compiler_params=params(32, "arbitrary"),
        cost_estimate=cost(flops, keys.size * 8),
        name="run_layers",
    )(x, *shared)


def local(
    table,
    history,
    lengths,
    assignment,
    cand_owner,
    cand_row,
    norm_gain,
    w_query,
    w_key,
    attn_gain,
    w_out,
):
    groups = lax.axis_size("gy")
    members = lax.axis_size("gx")
    count = cand_row.shape[0]
    rows, features = table.shape
    capacity = 2 * count // groups
    fast_cap = 5 * capacity // 8
    first_cap = capacity // 3
    tile = count // 4
    first_count = 3 * tile

    layers, _, span, _ = history.shape
    owner = cand_owner.reshape(1, count)
    row = cand_row.reshape(1, count)
    block = jax.ShapeDtypeStruct((layers, span, features), BF16)
    others = members - 1
    vmem, smem = pl.BlockSpec(memory_space=pltpu.VMEM), pl.BlockSpec(memory_space=pltpu.SMEM)
    hbm = pl.BlockSpec(memory_space=pltpu.HBM)
    requests, rank, *sent = pl.pallas_call(
        functools.partial(requests_kernel, rows, members, fast_cap, first_cap, first_count),
        in_specs=[vmem, vmem, smem, hbm],
        out_specs=[vmem, vmem] + [hbm] * others,
        out_shape=[
            jax.ShapeDtypeStruct((groups, 1, capacity + LANES), jnp.int32),
            jax.ShapeDtypeStruct((1, count), jnp.int32),
        ]
        + [block] * others,
        scratch_shapes=[
            pltpu.VMEM((others, layers, span, features), BF16),
            pltpu.SemaphoreType.DMA((others,)),
            pltpu.SemaphoreType.DMA((others,)),
        ],
        compiler_params=params(16),
        cost_estimate=cost(8 * count * count, 1),
        name="requests",
    )(owner, row, assignment, history)

    def exchange(block):
        return lax.all_to_all(block, "gy", split_axis=0, concat_axis=0, tiled=True)

    ids = exchange(requests)
    blocks = [
        lax.ppermute(block, "gx", [(j, (j + shift) % members) for j in range(members)])
        for shift, block in enumerate(sent, 1)
    ]
    slow = jnp.any(ids[:, 0, capacity] > 0)
    pos, slots = pl.pallas_call(
        functools.partial(order_kernel, groups, fast_cap, first_cap),
        out_shape=[jax.ShapeDtypeStruct((count, 1), F32)] * 2,
        compiler_params=params(12),
        cost_estimate=cost(8 * count * count, 1),
        name="order",
    )(owner, rank)

    second_cap = fast_cap - first_cap
    found_1 = lookup(ids, table, norm_gain, 0, first_cap)
    arrived_1 = exchange(found_1)
    found_2 = lookup(ids, table, slots, first_cap, second_cap)
    arrived_2 = exchange(found_2)
    arrived_1 = arrived_1.reshape(groups * first_cap, features)
    arrived_2 = arrived_2.reshape(groups * second_cap, features)
    keys, values = project(assignment, lengths, history, blocks, norm_gain, w_key)
    shared = (keys, values, norm_gain, w_query, attn_gain, w_out)
    early = run_layers(pick(slots, (arrived_1,), 0, 0, first_count, tile), tile, *shared)
    placed = pick(pos, (early,), 0, 0, count, tile)
    late = pick(
        slots, (arrived_1, arrived_2), 0, first_count, count - first_count, tile, after=placed
    )
    late = run_layers(late, tile, *shared)

    def in_order(operands):
        pos, placed, late = operands
        return pick(pos, (late,), first_count, 0, count, tile, placed)

    def in_full(operands):
        arrived = exchange(jnp.take(table, ids[:, 0, :capacity], axis=0, mode="clip"))
        place = (owner * capacity + rank).reshape(count)
        embedded = jnp.take(arrived.reshape(groups * capacity, features), place, axis=0, mode="clip")
        return run_layers(embedded, tile, *shared)

    return lax.cond(slow, in_full, in_order, (pos, placed, late))


def solution(mesh):
    return jax.shard_map(
        local,
        mesh=mesh,
        in_specs=(
            P("gy", None),
            P(None, "gy", "gx", None),
            P("gy", None),
            P("gy", None),
            P(("gx", "gy"), None),
            P(("gx", "gy")),
            P(),
            P(),
            P(),
            P(),
            P(),
        ),
        out_specs=P(("gx", "gy"), None),
        check_vma=False,
    )
```

```python
import functools

import jax
import jax.numpy as jnp
from jax import lax
from jax.experimental import pallas as pl
from jax.experimental.pallas import tpu as pltpu
from jax.sharding import PartitionSpec as P


HEADS = 4
EPSILON = 1e-06
NT = (((1,), (1,)), ((), ()))
KEY_TILE = 256
LANES = 128
F32, BF16 = jnp.float32, jnp.bfloat16


def half_silu(half):
    return half + half * jnp.tanh(half)


def rms_scale(vector, gain_row):
    scale = lax.rsqrt(jnp.mean(vector * vector, axis=-1, keepdims=True) + EPSILON)
    return vector * scale * gain_row


def params(mib, *semantics):
    return pltpu.CompilerParams(
        dimension_semantics=semantics or None, vmem_limit_bytes=mib * 2**20
    )


def cost(flops, moved):
    return pl.CostEstimate(flops=int(flops), bytes_accessed=int(moved), transcendentals=0)


def iota(shape, axis):
    return lax.broadcasted_iota(jnp.int32, shape, axis).astype(F32)


def column(row):
    return jnp.broadcast_to(row, (8, row.shape[1])).T[:, 0:1]


def requests_kernel(
    rows,
    members,
    fast_cap,
    first_cap,
    first_count,
    owner_ref,
    row_ref,
    assignment_ref,
    history_ref,
    req_ref,
    rank_ref,
    *refs,
):
    sent, (held, read_sems, write_sems) = refs[: members - 1], refs[members - 1 :]
    own = lax.axis_index("gx")
    reads, writes = [], []
    for shift, out in enumerate(sent, 1):
        user = assignment_ref[0, lax.rem(own + shift, members)]
        block = held.at[shift - 1]
        reads.append(
            pltpu.make_async_copy(history_ref.at[:, user], block, read_sems.at[shift - 1])
        )
        writes.append(pltpu.make_async_copy(block, out, write_sems.at[shift - 1]))
    for copy in reads:
        copy.start()
    groups = req_ref.shape[0]
    capacity = req_ref.shape[2] - LANES
    count = owner_ref.shape[1]
    owner = owner_ref[...].astype(F32)
    row = row_ref[...].reshape(1, count).astype(F32)
    key = owner * rows + row
    keys = column(key)
    place = iota((1, count), 1)
    step = 128
    first = jnp.full((8, count), float(count), F32)
    for base in range(0, count, step):
        same = keys[base : base + step] == key
        at = jnp.where(same, iota((step, 1), 0) + base, float(count))
        first = jnp.minimum(first, jnp.min(at.reshape(step // 8, 8, count), axis=0))
    first = jnp.min(first, axis=0, keepdims=True)
    for read, write in zip(reads, writes):
        read.wait()
        write.start()
    owned = iota((groups, 1), 0) == owner
    leads = jnp.where(owned & (first == place), 1.0, 0.0)
    prior = jnp.zeros((groups, count), F32)
    step = 256
    for base in range(0, count, step):
        before = jnp.where(iota((step, 1), 0) + base < first, 1.0, 0.0).astype(BF16)
        prior += jnp.dot(
            leads[:, base : base + step].astype(BF16), before, preferred_element_type=F32
        )
    rank = jnp.sum(jnp.where(owned, prior, 0.0), axis=0, keepdims=True)
    high = jnp.floor(row * (1.0 / 256))
    low = row - high * 256
    parts = jnp.concatenate([leads * high, leads * low], axis=0).astype(BF16)
    at_slot = jnp.where(iota((capacity, 1), 0) == rank, 1.0, 0.0).astype(BF16)
    listed = lax.dot_general(parts, at_slot, NT, preferred_element_type=F32)
    asked = listed[:groups] * 256 + listed[groups:]
    most = jnp.max(jnp.sum(leads, axis=1, keepdims=True), axis=0, keepdims=True)
    ready = jnp.sum(jnp.where(rank < first_cap, 1.0, 0.0), axis=1, keepdims=True)
    slow = (most > fast_cap) | (ready < first_count)
    flag = jnp.broadcast_to(jnp.where(slow, 1, 0).astype(jnp.int32), (1, LANES))
    asked = asked.astype(jnp.int32)
    for g in range(groups):
        req_ref[g, :, :capacity] = asked[g : g + 1]
        req_ref[g, :, capacity:] = flag
    rank_ref[...] = rank.astype(jnp.int32)
    for write in writes:
        write.wait()


def order_kernel(groups, fast_cap, first_cap, owner_ref, rank_ref, pos_ref, slot_ref):
    count = owner_ref.shape[1]
    owner = owner_ref[...].astype(F32)
    rank = rank_ref[...].astype(F32)
    key = rank * count + iota((1, count), 1)
    keys = column(key)
    step = 128
    smaller = jnp.zeros((8, count), F32)
    for base in range(0, count, step):
        less = jnp.where(keys[base : base + step] < key, 1.0, 0.0)
        smaller += jnp.sum(less.reshape(step // 8, 8, count), axis=0)
    pos = jnp.sum(smaller, axis=0, keepdims=True)
    pos_ref[...] = column(pos)
    rest = fast_cap - first_cap
    slot = jnp.where(
        rank < first_cap,
        owner * first_cap + rank,
        groups * first_cap + owner * rest + (rank - first_cap),
    )
    for base in range(0, count, step):
        here = jnp.where(iota((step, 1), 0) + base == pos, slot, 0.0)
        slot_ref[base : base + step, :] = jnp.sum(here, axis=1, keepdims=True)


def lookup_kernel(offset, ids_ref, source_ref, _, out_ref, select, table_ref, sem):
    copy = pltpu.make_async_copy(source_ref, table_ref, sem)
    copy.start()
    groups, length, features = out_ref.shape
    lanes = iota((1, table_ref.shape[0]), 1)
    for g in range(groups):
        ids = column(ids_ref[g].astype(F32))[offset : offset + length]
        hit = jnp.where(ids == lanes, 1.0, 0.0)
        select[g * length : (g + 1) * length, :] = hit.astype(BF16)
    copy.wait()
    found = jnp.dot(select[...], table_ref[...], preferred_element_type=F32)
    out_ref[...] = found.astype(BF16).reshape(groups, length, features)


def lookup(ids, table, after, offset, length):
    groups = ids.shape[0]
    rows, features = table.shape
    part = (min(8, after.shape[0]), after.shape[1])
    return pl.pallas_call(
        functools.partial(lookup_kernel, offset),
        grid=(1,),
        in_specs=[
            pl.BlockSpec(ids.shape, lambda i: (0, 0, 0)),
            pl.BlockSpec(memory_space=pltpu.HBM),
            pl.BlockSpec(part, lambda i: (0, 0)),
        ],
        out_specs=pl.BlockSpec((groups, length, features), lambda i: (0, 0, 0)),
        out_shape=jax.ShapeDtypeStruct((groups, length, features), BF16),
        scratch_shapes=[
            pltpu.VMEM((groups * length, rows), BF16),
            pltpu.VMEM((rows, features), BF16),
            pltpu.SemaphoreType.DMA,
        ],
        compiler_params=params(44, "arbitrary"),
        cost_estimate=cost(2 * groups * length * rows * features, table.size * 2),
        name="lookup",
    )(ids, table, after)


def picked(slot, refs, base):
    total = None
    for ref in refs:
        size = ref.shape[0]
        hit = jnp.where(slot == iota((1, size), 1) + base, 1.0, 0.0).astype(BF16)
        found = jnp.dot(hit, ref[...], preferred_element_type=F32)
        total = found if total is None else total + found
        base += size
    return total


def pick_kernel(base, slot_ref, source_ref, *refs):
    out_ref = refs[-1]
    total = picked(slot_ref[...], (source_ref,), base)
    for ref in refs[:-1]:
        total = total + ref[...].astype(F32)
    out_ref[...] = total.astype(out_ref.dtype)


def pick(slots, source, base, tile, *addends):
    amount = slots.shape[0]
    size, features = source.shape
    row_block = pl.BlockSpec((tile, features), lambda i: (i, 0))
    return pl.pallas_call(
        functools.partial(pick_kernel, base),
        grid=(amount // tile,),
        in_specs=[
            pl.BlockSpec((tile, 1), lambda i: (i, 0)),
            pl.BlockSpec(source.shape, lambda i: (0, 0)),
        ]
        + [row_block] * len(addends),
        out_specs=row_block,
        out_shape=jax.ShapeDtypeStruct((amount, features), BF16),
        compiler_params=params(16, "arbitrary"),
        cost_estimate=cost(2 * amount * size * features, size * features * 2),
        name="pick",
    )(slots, source, *addends)


def project_kernel(members, assignment_ref, lengths_ref, history_ref, *refs):
    blocks = refs[: members - 1]
    gain_ref, weight_ref, key_ref, value_ref, own_block, sem = refs[members - 1 :]
    span, features = own_block.shape
    layer = pl.program_id(0)
    own = lax.axis_index("gx")
    user = assignment_ref[0, own]
    length = lengths_ref[0, user]
    copy = pltpu.make_async_copy(history_ref.at[layer, user], own_block, sem)
    copy.start()
    copy.wait()
    for shift in range(members):
        states = own_block[...] if shift == 0 else blocks[shift - 1][0]
        normed = rms_scale(states.astype(F32), gain_ref[0]).astype(BF16)
        half = 0.5 * jnp.dot(normed, weight_ref[0], preferred_element_type=F32)
        key_value = half_silu(half)
        start = pl.multiple_of(lax.rem(own - shift + members, members) * span, span)
        live = lax.broadcasted_iota(jnp.int32, (span, 1), 0) + start < length
        key_ref[0, pl.ds(start, span), :] = key_value[:, :features].astype(BF16)
        value = jnp.where(live, key_value[:, features:], 0.0)
        value_ref[0, pl.ds(start, span), :] = value.astype(BF16)


def project(assignment, lengths, history, blocks, gain, weight):
    layers, _, span, features = history.shape
    members = len(blocks) + 1
    per_layer = lambda *shape: pl.BlockSpec((1,) + shape, lambda i: (i, 0, 0))
    whole = jax.ShapeDtypeStruct((layers, span * members, features), BF16)
    return pl.pallas_call(
        functools.partial(project_kernel, members),
        grid=(layers,),
        in_specs=[
            pl.BlockSpec(memory_space=pltpu.SMEM),
            pl.BlockSpec(memory_space=pltpu.SMEM),
            pl.BlockSpec(memory_space=pltpu.HBM),
        ]
        + [per_layer(span, features)] * (members - 1)
        + [per_layer(1, features), per_layer(features, 2 * features)],
        out_specs=[per_layer(span * members, features)] * 2,
        out_shape=[whole] * 2,
        scratch_shapes=[pltpu.VMEM((span, features), BF16), pltpu.SemaphoreType.DMA],
        compiler_params=params(20, "arbitrary"),
        cost_estimate=cost(4 * layers * span * members * features**2, history.size * 4),
        name="project",
    )(assignment, lengths, history, *blocks, gain.reshape(layers, 1, features), weight)


def layers_kernel(count, slot_ref, *refs):
    sources, refs = refs[:count], refs[count:]
    keys_ref, values_ref, ng_ref, wq_ref, ag_ref, wo_ref = refs[:6]
    out_ref, key_ref, value_ref, sems = refs[-4:]
    layers, total, features = key_ref.shape
    opening = pl.program_id(0) == 0
    copies = [
        (
            pltpu.make_async_copy(keys_ref.at[layer], key_ref.at[layer], sems.at[2 * layer]),
            pltpu.make_async_copy(values_ref.at[layer], value_ref.at[layer], sems.at[2 * layer + 1]),
        )
        for layer in range(layers)
    ]

    @pl.when(opening)
    def _():
        for pair in copies:
            for copy in pair:
                copy.start()

    size = features // HEADS
    scale = 0.5 * size**-0.5
    x = picked(slot_ref[...], sources, 0)
    for layer in range(layers):
        normed = rms_scale(x, ng_ref[layer : layer + 1, :]).astype(BF16)
        weight = wq_ref[layer]
        gate = jnp.dot(normed, weight[:, :features], preferred_element_type=F32)
        gate = half_silu(0.5 * gate).astype(BF16)
        query = jnp.dot(normed, weight[:, features:], preferred_element_type=F32)
        query = (half_silu(0.5 * query) * scale).astype(BF16)

        @pl.when(opening)
        def _():
            for copy in copies[layer]:
                copy.wait()

        heads = []
        for head in range(HEADS):
            columns = slice(head * size, (head + 1) * size)
            attended = None
            for base in range(0, total, KEY_TILE):
                rows = slice(base, base + KEY_TILE)
                half = lax.dot_general(
                    query[:, columns],
                    key_ref[layer, rows, columns],
                    NT,
                    preferred_element_type=F32,
                )
                part = jnp.dot(
                    half_silu(half).astype(BF16),
                    value_ref[layer, rows, columns],
                    preferred_element_type=F32,
                )
                attended = part if attended is None else attended + part
            heads.append(attended)
        attended = rms_scale(jnp.concatenate(heads, axis=1), ag_ref[layer : layer + 1, :])
        gated = (attended * gate.astype(F32)).astype(BF16)
        x = x + jnp.dot(gated, wo_ref[layer], preferred_element_type=F32)
    out_ref[...] = x.astype(BF16)


def run_layers(slots, first, amount, sources, tile, shared, after=()):
    keys, _, _, _, _, _ = shared
    layers, total, features = keys.shape
    lead = first // tile
    full = lambda a: pl.BlockSpec(a.shape, lambda i: (0,) * a.ndim)
    held = pltpu.VMEM(keys.shape, BF16)
    flops = layers * amount * features * (6 * features + 8 * total)
    return pl.pallas_call(
        functools.partial(layers_kernel, len(sources)),
        grid=(amount // tile,),
        in_specs=[pl.BlockSpec((tile, 1), lambda i: (i + lead, 0))]
        + [full(a) for a in sources]
        + [pl.BlockSpec(memory_space=pltpu.HBM)] * 2
        + [full(a) for a in shared[2:]]
        + [pl.BlockSpec((16, features), lambda i: (0, 0))] * len(after),
        out_specs=pl.BlockSpec((tile, features), lambda i: (i, 0)),
        out_shape=jax.ShapeDtypeStruct((amount, features), BF16),
        scratch_shapes=[held, held, pltpu.SemaphoreType.DMA((2 * layers,))],
        compiler_params=params(40, "arbitrary"),
        cost_estimate=cost(flops, keys.size * 8),
        name="run_layers",
    )(slots, *sources, *shared, *after)


def local(
    table,
    history,
    lengths,
    assignment,
    cand_owner,
    cand_row,
    norm_gain,
    w_query,
    w_key,
    attn_gain,
    w_out,
):
    groups = lax.axis_size("gy")
    members = lax.axis_size("gx")
    count = cand_row.shape[0]
    rows, features = table.shape
    capacity = 2 * count // groups
    fast_cap = 5 * capacity // 8
    first_cap = 7 * capacity // 24
    tile = count // 4
    first_count = 3 * tile

    layers, _, span, _ = history.shape
    owner = cand_owner.reshape(1, count)
    block = jax.ShapeDtypeStruct((layers, span, features), BF16)
    others = members - 1
    vmem, smem = pl.BlockSpec(memory_space=pltpu.VMEM), pl.BlockSpec(memory_space=pltpu.SMEM)
    hbm = pl.BlockSpec(memory_space=pltpu.HBM)
    requests, rank, *sent = pl.pallas_call(
        functools.partial(requests_kernel, rows, members, fast_cap, first_cap, first_count),
        in_specs=[vmem, vmem, smem, hbm],
        out_specs=[vmem, vmem] + [hbm] * others,
        out_shape=[
            jax.ShapeDtypeStruct((groups, 1, capacity + LANES), jnp.int32),
            jax.ShapeDtypeStruct((1, count), jnp.int32),
        ]
        + [block] * others,
        scratch_shapes=[
            pltpu.VMEM((others, layers, span, features), BF16),
            pltpu.SemaphoreType.DMA((others,)),
            pltpu.SemaphoreType.DMA((others,)),
        ],
        compiler_params=params(60),
        cost_estimate=cost(8 * count * count, 1),
        name="requests",
    )(owner, cand_row, assignment, history)

    def exchange(block):
        return lax.all_to_all(block, "gy", split_axis=0, concat_axis=0, tiled=True)

    ids = exchange(requests)
    blocks = [
        lax.ppermute(block, "gx", [(j, (j + shift) % members) for j in range(members)])
        for shift, block in enumerate(sent, 1)
    ]
    slow = jnp.any(ids[:, 0, capacity] > 0)
    pos, slots = pl.pallas_call(
        functools.partial(order_kernel, groups, fast_cap, first_cap),
        out_shape=[jax.ShapeDtypeStruct((count, 1), F32)] * 2,
        compiler_params=params(12),
        cost_estimate=cost(8 * count * count, 1),
        name="order",
    )(owner, rank)

    second_cap = fast_cap - first_cap
    found_1 = lookup(ids, table, norm_gain, 0, first_cap)
    arrived_1 = exchange(found_1)
    found_2 = lookup(ids, table, slots, first_cap, second_cap)
    arrived_2 = exchange(found_2)
    arrived_1 = arrived_1.reshape(groups * first_cap, features)
    arrived_2 = arrived_2.reshape(groups * second_cap, features)
    keys, values = project(assignment, lengths, history, blocks, norm_gain, w_key)
    shared = (keys, values, norm_gain, w_query, attn_gain, w_out)
    early = run_layers(slots, 0, first_count, (arrived_1,), tile, shared)
    placed = pick(pos, early, 0, tile)
    late_count = count - first_count
    late = run_layers(
        slots, first_count, late_count, (arrived_1, arrived_2), tile, shared, (placed,)
    )

    def in_order(operands):
        pos, placed, late = operands
        return pick(pos, late, first_count, tile, placed)

    def in_full(operands):
        arrived = exchange(jnp.take(table, ids[:, 0, :capacity], axis=0, mode="clip"))
        place = (owner * capacity + rank).reshape(count)
        embedded = jnp.take(arrived.reshape(groups * capacity, features), place, axis=0, mode="clip")
        every = jnp.arange(count, dtype=F32).reshape(count, 1)
        return run_layers(every, 0, count, (embedded,), tile // 4, shared)

    return lax.cond(slow, in_full, in_order, (pos, placed, late))


def solution(mesh):
    return jax.shard_map(
        local,
        mesh=mesh,
        in_specs=(
            P("gy", None),
            P(None, "gy", "gx", None),
            P("gy", None),
            P("gy", None),
            P(("gx", "gy"), None),
            P(("gx", "gy")),
            P(),
            P(),
            P(),
            P(),
            P(),
        ),
        out_specs=P(("gx", "gy"), None),
        check_vma=False,
    )
```
